256 devices in a mesh: section: 2 (over y_hi), dp: 16 (over z, core), vocab: 8 (over y_lo, x).
Axes of the slice: x: 4, y: 4 (y_hi: 2, y_lo: 2; y = y_hi * 2 + y_lo), z: 8, core: 2. Of those that a mesh axis runs over, the one named last changes fastest.
Arguments:
- activations: bfloat16 [2, 2048, 2048], P('section', 'dp'), may hold values from -32 to 32
- token_ids: int32 [2, 2048], replicated, may hold values from 0 to 65535
- embed_table: bfloat16 [65536, 2048], P(('dp', 'vocab')), may hold values from -3 to 3
Outputs:
- tied_grad: bfloat16 [128, 2, 256, 2048], P(('dp', 'vocab'), 'section')
The draws below stay inside these ranges and needn't reach their ends.
All inputs are finite; a program needn't handle non-finite values.
Results may differ from the reference program's by a relative error of at most 0.0029.
Values may be sent and summed in bfloat16 or wider, within the bound.
No kernel may reach another device: no remote copies, remote signals or barrier semaphores. Data moves between devices by JAX's collectives and lax.ppermute only.
A program may use at most 128 MiB of HBM per device.

```python
import math
import jax
import jax.numpy as jnp
import numpy as np
from jax import lax

D = 2048
VOCAB_DEV = 512
TOKENS = 2048
VOCAB = 65536
N_SECTION = 2


def table_rows(key, row_numbers):
    base_key = jax.random.fold_in(key, 101)

    def one_row(row_index):
        values = jax.random.normal(jax.random.fold_in(base_key, row_index), (D,), jnp.float32)
        return jnp.clip(values * (4.0 / math.sqrt(D)), -3.0, 3.0)
    return jax.vmap(one_row)(row_numbers)


def draw_embed_table(key, part):
    return table_rows(key, jnp.arange(VOCAB, dtype=jnp.int32)).astype(jnp.bfloat16)


def draw_activations(key, part):
    draw_key = jax.random.fold_in(key, 202)
    values = jax.random.normal(draw_key, (N_SECTION, TOKENS, D), jnp.float32)
    return jnp.clip(values, -32.0, 32.0).astype(jnp.bfloat16)


def plant(entries, stream_key, smallest, largest):
    spot = [jax.random.randint(jax.random.fold_in(stream_key, axis), (), 0, length) for axis, length in enumerate(entries.shape)]
    widest = entries.shape.index(max(entries.shape))
    beside = spot[:widest] + [(spot[widest] + 1) % entries.shape[widest]] + spot[widest + 1:]
    return entries.at[tuple(spot)].set(smallest).at[tuple(beside)].set(largest)


def rank_table(number_of, lean):
    portions = [(1 << 20) // math.isqrt(standing ** lean) + 1 for standing in range(1, number_of + 1)]
    scale = 1 + sum(portions) // (1 << 30)
    return np.cumsum(np.array([max(1, weight // scale) for weight in portions]))


def ranked(stream_key, shape, count, slope):
    listing = rank_table(count, slope)
    pick = jax.random.randint(jax.random.fold_in(stream_key, 1), shape, 0, int(listing[count - 1]))
    grade = jnp.searchsorted(jnp.asarray(listing, jnp.int32), pick, side="right")
    return jax.random.permutation(jax.random.fold_in(stream_key, 2), count)[grade].astype(jnp.int32)


def setup_inputs(seed: int = 0) -> dict:
    arg_keys = jax.random.split(jax.random.key(seed), 4)
    return {
        "activations": draw_activations(jax.random.fold_in(arg_keys[3], 71), 0),
        "token_ids": plant(ranked(arg_keys[1], (N_SECTION, TOKENS), VOCAB, 1), jax.random.fold_in(arg_keys[1], 3), 0, VOCAB - 1).astype(jnp.int32),
        "embed_table": draw_embed_table(jax.random.fold_in(arg_keys[3], 71), 0),
    }


def reference(activations, token_ids, embed_table):
    cotangent = activations[0]
    hidden = activations[1]
    input_ids = token_ids[0]
    target_ids = token_ids[1]
    blocks = embed_table.shape[0] // VOCAB_DEV
    table_blocks = embed_table.reshape(blocks, VOCAB_DEV, D)
    offsets = jnp.arange(blocks, dtype=jnp.int32) * VOCAB_DEV
    columns = jnp.arange(VOCAB_DEV, dtype=jnp.int32)

    def scores(table_slab):
        return jnp.dot(hidden, table_slab.T, preferred_element_type=jnp.float32)

    def running(state_pair, table_slab):
        row_peak, row_total = state_pair
        logits = scores(table_slab)
        new_peak = jnp.maximum(row_peak, jnp.max(logits, axis=1))
        row_total = row_total * jnp.exp(row_peak - new_peak) + jnp.sum(jnp.exp(logits - new_peak[:, None]), axis=1)
        return (new_peak, row_total), None

    initial = (jnp.full((TOKENS,), -1e30, jnp.float32), jnp.zeros((TOKENS,), jnp.float32))
    (row_peak, row_total), _ = lax.scan(running, initial, table_blocks)

    def block_gradient(block_pair):
        table_slab, offset = block_pair
        logits = scores(table_slab)
        target_hot = (target_ids[:, None] == offset + columns[None, :]).astype(jnp.float32)
        input_hot = (input_ids[:, None] == offset + columns[None, :]).astype(jnp.bfloat16)
        last_section = (jnp.exp(logits - row_peak[:, None]) / row_total[:, None] - target_hot).astype(jnp.bfloat16)
        gradient = jnp.dot(last_section.T, hidden, preferred_element_type=jnp.float32)
        gradient = gradient + jnp.dot(input_hot.T, cotangent, preferred_element_type=jnp.float32)
        return gradient.astype(jnp.bfloat16)

    gradients = lax.map(block_gradient, (table_blocks, offsets))
    return gradients.reshape(blocks, N_SECTION, VOCAB_DEV // N_SECTION, D)
```

```python
import jax
import jax.numpy as jnp
import numpy as np
from jax import lax
from jax.sharding import Mesh
from jax.sharding import PartitionSpec as P

AXES = ("s", "z", "c", "u", "x")
SUBS = 2
SLOTS = 8


def sizes():
    return {a: lax.axis_size(a) for a in AXES}


def moved(block, route):
    n = sizes()
    shape = [n[a] for a in AXES]
    pairs = []
    for at in np.ndindex(*shape):
        to = route(dict(zip(AXES, at)))
        to = tuple(to[a] % n[a] for a in AXES)
        pairs.append((int(np.ravel_multi_index(at, shape)), int(np.ravel_multi_index(to, shape))))
    return lax.ppermute(block, AXES, pairs)


def across(d):
    return {**d, "s": 1 - d["s"], "u": 1 - d["u"]}


def along_z(d):
    return {**d, "z": d["z"] + (1 if (d["x"] + d["c"]) % 2 == 0 else -1)}


def along_x(d):
    return {**d, "x": d["x"] + (-1 if d["c"] == 0 else 1)}


def other_core(d):
    return {**d, "c": 1 - d["c"]}


def plus_z(d):
    return {**d, "z": d["z"] + 1}


def picked(table, index):
    hit = index[:, None] == jnp.arange(table.shape[0], dtype=jnp.int32)[None, :]
    hit = hit.reshape(hit.shape + (1,) * (table.ndim - 1))
    return jnp.sum(jnp.where(hit, table[None], jnp.zeros((), table.dtype)), axis=1)


def shared(value, axes):
    count = lax.axis_size(axes)
    return lax.all_to_all(jnp.broadcast_to(value, (count, *value.shape)), axes, 0, 0, tiled=True)


def joined(pairs):
    peak = jnp.max(pairs[:, 0], axis=0)
    total = jnp.sum(pairs[:, 1] * jnp.exp(pairs[:, 0] - peak[None]), axis=0)
    return jnp.stack([peak, total])


def dot(a, b, dims):
    return lax.dot_general(a, b, (dims, ((), ())), preferred_element_type=jnp.float32)


def body(activations, token_ids, embed_table):
    own_rows = activations[0]
    rows, width = own_rows.shape
    n = sizes()
    nz, nc = n["z"], n["c"]
    s, z, c, u, x = (lax.axis_index(a) for a in AXES)
    column = u * n["x"] + x
    columns = n["u"] * n["x"]
    table_count = embed_table.shape[0]
    half = table_count // n["s"]

    mine = lax.dynamic_slice_in_dim(embed_table, s * half, half, 0)
    theirs = moved(mine, other_core)
    pool = jnp.concatenate([theirs, mine], axis=0)

    cut = rows // SUBS
    blocks, cots = [], []
    for k in range(SUBS):
        piece = own_rows[k * cut : (k + 1) * cut]
        partner = moved(piece, across)
        blocks.append(jnp.where(s == 0, partner, piece))
        cots.append(jnp.where(s == 0, piece, partner))
    cot = jnp.concatenate(cots, axis=0)

    there = [[b] for b in blocks]
    back = [[] for _ in blocks]
    for step in range(1, nz // 2 + 1):
        for k in range(SUBS):
            there[k].append(moved(there[k][-1], along_z))
        if step > 1:
            for k in range(SUBS):
                back[k].append(moved(there[k][step - 1], along_x))
    pieces = []
    for q in range(nz):
        for k in range(SUBS):
            pieces.append(there[k][q] if q <= nz // 2 else back[k][nz - q - 1])
    hid = jnp.concatenate(pieces, axis=0)

    way = jnp.where((x + c) % 2 == 0, 1, -1)
    order = (z - way * jnp.arange(nz, dtype=jnp.int32)) % nz
    ids = token_ids.reshape(2, nz, nc, rows)
    ids = jnp.sum(jnp.where(jnp.arange(nc)[None, None, :, None] == c, ids, 0), axis=2)
    targets = picked(ids[1], order).reshape(1, nz * rows)

    base = lambda core: ((z * nc + core) * columns + column) * table_count + s * half
    line = jnp.arange(2 * half, dtype=jnp.int32)
    pool_rows = jnp.where(line < half, base(1 - c) + line, base(c) + line - half)

    per_z = nc * columns * table_count
    cell_of = lambda v: (v // per_z, (v // table_count) % columns, (v // half) % n["s"])
    before = (
        jnp.arange(rows)[:, None] < jnp.arange(rows)[None, :]
    ).astype(jnp.bfloat16)

    def ranks(match):
        return dot(match.astype(jnp.bfloat16), before, ((1,), (0,))).astype(jnp.int32)

    slot = jnp.arange(SLOTS, dtype=jnp.int32)
    shard_ids = picked(ids[0], z[None])[0]
    to_z, to_column, to_s = cell_of(shard_ids)
    here = (to_column == column) & (to_s == s)
    out_match = (to_z[None, :] == jnp.arange(nz)[:, None]) & here[None, :]
    out_rank = ranks(out_match)
    choose = out_match[:, None, :] & (out_rank[:, None, :] == slot[None, :, None])
    sent = dot(choose.reshape(nz * SLOTS, rows).astype(jnp.bfloat16), cot, ((1,), (0,)))
    got = lax.all_to_all(sent.astype(jnp.bfloat16), "z", 0, 0, tiled=True)
    from_z, from_column, from_s = cell_of(ids[0])
    in_match = (from_z == z) & (from_column == column) & (from_s == s)
    in_rank = ranks(in_match)
    filled = in_match[:, None, :] & (in_rank[:, None, :] == slot[None, :, None])
    slot_row = jnp.sum(jnp.where(filled, ids[0][:, None, :] + 1, 0), axis=2) - 1
    first_part = (pool_rows[:, None] == slot_row.reshape(1, -1)).astype(jnp.bfloat16)

    every = token_ids[0].reshape(nz * nc, rows)
    cz, cc, cs = cell_of(every)
    cell = (cz * columns + cc) * n["s"] + cs
    cells = nz * columns * n["s"]
    held = jnp.sum(
        (cell[:, :, None] == jnp.arange(cells, dtype=jnp.int32)[None, None, :]).astype(jnp.int32), axis=1
    )
    crowded = jnp.max(held) > SLOTS

    logits = dot(pool, hid, ((1,), (1,)))
    peak = jnp.max(logits, axis=0)
    total = jnp.sum(jnp.exp(logits - peak[None]), axis=0)
    local = jnp.stack([peak, total]).reshape(2, nz, rows)
    inverse = (way * (z - jnp.arange(nz, dtype=jnp.int32))) % nz
    pair = jnp.stack([picked(local[0], inverse), picked(local[1], inverse)])
    pair = joined(shared(pair, ("s", "u", "x")))
    pair = joined(shared(pair, "z"))
    peak_all = picked(pair[0], order).reshape(1, nz * rows)
    total_all = picked(pair[1], order).reshape(1, nz * rows)

    hot = (pool_rows[:, None] == targets).astype(jnp.float32)
    last_part = (jnp.exp(logits - peak_all) / total_all - hot).astype(jnp.bfloat16)

    def gradient(lo):
        part = dot(last_part[lo : lo + half], hid, ((1,), (0,)))
        return part + dot(first_part[lo : lo + half], got, ((1,), (0,)))

    for_them = moved(gradient(0), other_core)
    for_us = gradient(half)

    def plain(for_us, for_them, cot, token_ids):
        return (for_us + for_them).astype(jnp.bfloat16)

    def crowded_too(for_us, for_them, cot, token_ids):
        my_rows = base(c) + jnp.arange(half, dtype=jnp.int32)

        def step(k, carry):
            total, block = carry
            shard = (z - k) % nz
            for core in range(2):
                if core == 1:
                    block = moved(block, other_core)
                owner = c if core == 0 else 1 - c
                shard_ids = lax.dynamic_slice(
                    token_ids[0].reshape(nz, nc, rows), (shard, owner, 0), (1, 1, rows)
                ).reshape(rows)
                a, b, d = cell_of(shard_ids)
                match = (a == z) & (b == column) & (d == s)
                late = match & (ranks(match[None])[0] >= SLOTS)
                weights = (my_rows[:, None] == jnp.where(late, shard_ids, -1)[None, :]).astype(jnp.bfloat16)
                total = total + dot(weights, block, ((1,), (0,)))
            block = moved(moved(block, other_core), plus_z)
            return total, block

        total, _ = lax.fori_loop(0, nz, step, (for_us + for_them, cot))
        return total.astype(jnp.bfloat16)

    out = lax.cond(crowded, crowded_too, plain, for_us, for_them, cot, token_ids)
    return out.reshape(1, 1, half, width)


def solution(mesh):
    finer = Mesh(mesh.devices.reshape(mesh.shape["section"], 8, 2, 2, 4), AXES)
    in_specs = (P("s", ("z", "c"), None), P(), P(("z", "c", "u", "x"), None))
    out_specs = P(("z", "c", "u", "x"), "s", None, None)
    return jax.shard_map(body, mesh=finer, in_specs=in_specs, out_specs=out_specs, check_vma=False)
```

```python
import jax
import jax.numpy as jnp
import numpy as np
from jax import lax
from jax.experimental import pallas as pl
from jax.experimental.pallas import tpu as pltpu
from jax.sharding import Mesh
from jax.sharding import PartitionSpec as P


AXES = ("s", "z", "c", "u", "x")
SUBS = 2
SLOTS = 8
CHUNK = 512


def sizes():
    return {a: lax.axis_size(a) for a in AXES}


def moved(block, route):
    n = sizes()
    shape = [n[a] for a in AXES]
    pairs = []
    for at in np.ndindex(*shape):
        to = route(dict(zip(AXES, at)))
        to = tuple(to[a] % n[a] for a in AXES)
        pairs.append((int(np.ravel_multi_index(at, shape)), int(np.ravel_multi_index(to, shape))))
    return lax.ppermute(block, AXES, pairs)


def across(d):
    return {**d, "s": 1 - d["s"], "u": 1 - d["u"]}


def along_z(d):
    return {**d, "z": d["z"] + (1 if (d["x"] + d["c"]) % 2 == 0 else -1)}


def along_x(d):
    return {**d, "x": d["x"] + (-1 if d["c"] == 0 else 1)}


def other_core(d):
    return {**d, "c": 1 - d["c"]}


def plus_z(d):
    return {**d, "z": d["z"] + 1}


def picked(table, index):
    hit = index[:, None] == jnp.arange(table.shape[0], dtype=jnp.int32)[None, :]
    hit = hit.reshape(hit.shape + (1,) * (table.ndim - 1))
    return jnp.sum(jnp.where(hit, table[None], jnp.zeros((), table.dtype)), axis=1)


def shared(value, axes):
    count = lax.axis_size(axes)
    return lax.all_to_all(jnp.broadcast_to(value, (count, *value.shape)), axes, 0, 0, tiled=True)


def joined(pairs):
    peak = jnp.max(pairs[:, 0], axis=0)
    total = jnp.sum(pairs[:, 1] * jnp.exp(pairs[:, 0] - peak[None]), axis=0)
    return jnp.stack([peak, total])


def dot(a, b, dims):
    return lax.dot_general(a, b, (dims, ((), ())), preferred_element_type=jnp.float32)


def anywhere(count):
    return [pl.BlockSpec(memory_space=pl.ANY)] * count


def in_vmem(count):
    return [pl.BlockSpec(memory_space=pltpu.VMEM)] * count


def fetch(sources, targets, sems):
    copies = [pltpu.make_async_copy(a, b, sems.at[k]) for k, (a, b) in enumerate(zip(sources, targets))]
    for copy in copies:
        copy.start()
    return copies


def await_rows(ref, each, count, k, sems, first):
    for j in range(count):
        piece = k * count + j
        view = ref.at[pl.ds(pl.multiple_of(piece * each, each), each), :]
        pltpu.make_async_copy(view, view, sems.at[first + piece]).wait()


def stacked(ref, parts):
    at, views = 0, []
    for part in parts:
        views.append(ref.at[pl.ds(at, part.shape[0]), :])
        at += part.shape[0]
    return views


def score_kernel(count, refs):
    start, table, parts = refs[0], refs[1], refs[2 : 2 + count]
    scores, stats, table_here, rows_here, sems = refs[2 + count :]
    lines = table_here.shape[0]
    mine = table.at[pl.ds(pl.multiple_of(start[0], lines), lines), :]
    copies = fetch([mine, *parts], [table_here, *stacked(rows_here, parts)], sems)
    copies[0].wait()
    each = parts[0].shape[0]

    def step(k, carry):
        await_rows(rows_here, each, CHUNK // each, k, sems, 1)
        at = pl.ds(pl.multiple_of(k * CHUNK, CHUNK), CHUNK)
        value = lax.dot_general(
            table_here[...], rows_here[at, :], (((1,), (1,)), ((), ())), preferred_element_type=jnp.float32
        )
        scores[:, at] = value
        peak = jnp.max(value, axis=0, keepdims=True)
        stats[0:1, at] = peak
        stats[1:2, at] = jnp.sum(jnp.exp(value - peak), axis=0, keepdims=True)
        return carry

    lax.fori_loop(0, rows_here.shape[0] // CHUNK, step, 0)


def scored(start, lines, table, parts):
    count = sum(p.shape[0] for p in parts)
    width = table.shape[1]
    return pl.pallas_call(
        lambda *refs: score_kernel(len(parts), refs),
        out_shape=[
            jax.ShapeDtypeStruct((lines, count), jnp.float32),
            jax.ShapeDtypeStruct((2, count), jnp.float32),
        ],
        in_specs=[pl.BlockSpec(memory_space=pltpu.SMEM)] + anywhere(1 + len(parts)),
        out_specs=in_vmem(2),
        scratch_shapes=[
            pltpu.VMEM((lines, width), table.dtype),
            pltpu.VMEM((count, width), table.dtype),
            pltpu.SemaphoreType.DMA((1 + len(parts),)),
        ],
        cost_estimate=pl.CostEstimate(
            flops=2 * count * lines * width, bytes_accessed=2 * width * (lines + count), transcendentals=0
        ),
        name="score",
    )(start.reshape(1), table, *parts)


def gradient_kernel(tables, count, refs):
    base, peak, total, targets, slots = refs[:5]
    gots, scores = refs[5:7], refs[7 : 7 + tables]
    parts = refs[7 + tables : 7 + tables + count]
    out, scores_here, rows_here, got_here, result, outgoing, sems = refs[7 + tables + count :]
    lines, width = out.shape
    at, views = 0, []
    for table in scores:
        views.append(scores_here.at[:, pl.ds(at, table.shape[1])])
        at += table.shape[1]
    copies = fetch(
        [*scores, *gots, *parts], views + stacked(got_here, gots) + stacked(rows_here, parts), sems
    )
    for copy in copies[: tables + 2]:
        copy.wait()
    row = base[0] + lax.broadcasted_iota(jnp.int32, (lines, 1), 0)
    first = jnp.where(row == slots[...], 1.0, 0.0).astype(got_here.dtype)
    span = outgoing.shape[2]
    columns = [slice(k * span, (k + 1) * span) for k in range(width // span)]
    for cols in columns:
        result[:, cols] = jnp.dot(first, got_here[:, cols], preferred_element_type=jnp.float32)
    each = parts[0].shape[0]

    def step(k, carry):
        await_rows(rows_here, each, CHUNK // each, k, sems, tables + 2)
        at = pl.ds(pl.multiple_of(k * CHUNK, CHUNK), CHUNK)
        hot = jnp.where(row == targets[:, at], 1.0, 0.0)
        soft = jnp.exp(scores_here[:, at] - peak[:, at]) * (1.0 / total[:, at])
        weights = (soft - hot).astype(rows_here.dtype)
        for cols in columns:
            result[:, cols] += jnp.dot(weights, rows_here[at, cols], preferred_element_type=jnp.float32)
        return carry

    lax.fori_loop(0, rows_here.shape[0] // CHUNK, step, 0)
    stores = []
    for k, cols in enumerate(columns):
        outgoing[k] = result[:, cols].astype(out.dtype)
        store = pltpu.make_async_copy(
            outgoing.at[k], out.at[:, pl.ds(k * span, span)], sems.at[len(copies) + k]
        )
        store.start()
        stores.append(store)
    for store in stores:
        store.wait()


def gradient(dtype, lines, base, scores, parts, peak, total, targets, slots, gots):
    tokens, width = peak.shape[1], gots[0].shape[1]
    step = width // 4
    return pl.pallas_call(
        lambda *refs: gradient_kernel(len(scores), len(parts), refs),
        out_shape=jax.ShapeDtypeStruct((lines, width), dtype),
        in_specs=[pl.BlockSpec(memory_space=pltpu.SMEM)] + in_vmem(4) + anywhere(2 + len(scores) + len(parts)),
        out_specs=pl.BlockSpec(memory_space=pl.ANY),
        scratch_shapes=[
            pltpu.VMEM((lines, tokens), jnp.float32),
            pltpu.VMEM((tokens, width), jnp.bfloat16),
            pltpu.VMEM((2 * gots[0].shape[0], width), jnp.bfloat16),
            pltpu.VMEM((lines, width), jnp.float32),
            pltpu.VMEM((width // step, lines, step), dtype),
            pltpu.SemaphoreType.DMA((2 + len(scores) + len(parts) + width // step,)),
        ],
        cost_estimate=pl.CostEstimate(
            flops=2 * tokens * lines * width, bytes_accessed=2 * width * tokens, transcendentals=lines * tokens
        ),
        name="gradient",
    )(base.reshape(1), peak, total, targets, slots, *gots, *scores, *parts)


def whole(activations, token_ids, embed_table):
    own_rows = activations[0]
    rows, width = own_rows.shape
    n = sizes()
    nz, nc = n["z"], n["c"]
    s, z, c, u, x = (lax.axis_index(a) for a in AXES)
    column = u * n["x"] + x
    columns = n["u"] * n["x"]
    table_count = embed_table.shape[0]
    half = table_count // n["s"]

    cut = rows // SUBS
    blocks, cots = [], []
    for k in range(SUBS):
        piece = own_rows[k * cut : (k + 1) * cut]
        partner = moved(piece, across)
        if blocks:
            partner, blocks[-1] = lax.optimization_barrier((partner, blocks[-1]))
        blocks.append(jnp.where(s == 0, partner, piece))
        cots.append(jnp.where(s == 0, piece, partner))
    cot = jnp.concatenate(cots, axis=0)

    hops = np.array([0, 1] + [h for step in range(2, nz // 2 + 1) for h in (step, 1 - step)], np.int32)
    way = jnp.where((x + c) % 2 == 0, 1, -1)
    order = []
    for k in range(0, len(hops), 2):
        near = hops[k : k + 2]
        order += [(z - way * near) % nz, (z + way * near) % nz + nz]
    order = jnp.concatenate(order)
    shards = nz * nc

    def both_cores(table):
        table = table.reshape(nz, nc, rows)
        mine = jnp.arange(nc, dtype=jnp.int32)[None, :, None] == c
        return jnp.concatenate(
            [jnp.sum(jnp.where(hit, table, 0), axis=1) for hit in (mine, ~mine)], axis=0
        )

    shard_in, shard_out = both_cores(token_ids[0].reshape(shards, rows)), both_cores(
        token_ids[1].reshape(shards, rows)
    )
    targets = picked(shard_out, order).reshape(1, shards * rows)
    base = ((z * nc + c) * columns + column) * table_count + s * half

    per_z = nc * columns * table_count
    cell_of = lambda v: (v // per_z, (v // table_count) % columns, (v // half) % n["s"])
    before = (
        jnp.arange(rows)[:, None] < jnp.arange(rows)[None, :]
    ).astype(jnp.bfloat16)

    def ranks(match):
        return dot(match.astype(jnp.bfloat16), before, ((1,), (0,))).astype(jnp.int32)

    slot = jnp.arange(SLOTS, dtype=jnp.int32)
    shard_ids = picked(shard_in[:nz], z[None])[0]
    to_z, to_column, to_s = cell_of(shard_ids)
    here = (to_column == column) & (to_s == s)
    out_match = (to_z[None, :] == jnp.arange(nz)[:, None]) & here[None, :]
    out_rank = ranks(out_match)
    every = token_ids[0].reshape(nz * nc, rows)
    cz, cc, cs = cell_of(every)
    cell = (cz * columns + cc) * n["s"] + cs
    cells = nz * columns * n["s"]
    held = jnp.sum(
        (cell[:, :, None] == jnp.arange(cells, dtype=jnp.int32)[None, None, :]).astype(jnp.int32), axis=1
    )
    crowded = jnp.max(held) > SLOTS

    cot, crowded = lax.optimization_barrier((cot, crowded))
    choose = out_match[:, None, :] & (out_rank[:, None, :] == slot[None, :, None])
    sent = dot(choose.reshape(nz * SLOTS, rows).astype(jnp.bfloat16), cot, ((1,), (0,)))
    sent = sent.astype(jnp.bfloat16)
    from_z, from_column, from_s = cell_of(shard_in)
    in_match = (from_z == z) & (from_column == column) & (from_s == s)
    in_rank = ranks(in_match)
    filled = in_match[:, None, :] & (in_rank[:, None, :] == slot[None, :, None])
    slots = jnp.sum(jnp.where(filled, shard_in[:, None, :] + 1, 0), axis=2).reshape(1, shards * SLOTS) - 1

    got = lax.all_to_all(sent, "z", 0, 0, tiled=True)

    there, back = [[block] for block in blocks], [[] for _ in blocks]
    for step in range(1, nz // 2 + 1):
        for k in range(SUBS):
            block = there[k][-1]
            there[k].append(moved(block, along_z))
            if step > 1:
                back[k].append(moved(block, along_x))
    parts = []
    for pair in range(0, len(hops), 2):
        group = []
        for hop in hops[pair : pair + 2]:
            group += [there[k][hop] if hop >= 0 else back[k][-hop - 1] for k in range(SUBS)]
        parts += group + [moved(p, other_core) for p in group]
    table_scores, stats = scored(s * half, half, embed_table, parts)
    stats, got = lax.optimization_barrier((stats, got))
    scores = [table_scores]
    gots = (got, moved(got, other_core))

    local = stats.reshape(2, shards, rows)
    place = jnp.arange(shards, dtype=jnp.int32)
    inverse = jnp.sum(jnp.where(order[None, :] == place[:, None], place[None, :], 0), axis=1)
    near = jnp.stack([picked(local[0], inverse[:nz]), picked(local[1], inverse[:nz])])
    far = jnp.stack([picked(local[0], inverse[nz:]), picked(local[1], inverse[nz:])])
    pair = joined(jnp.stack([near, moved(far, other_core)]))
    pair = joined(shared(pair, ("s", "u", "x")))
    pair = joined(shared(pair, "z"))
    pair = jnp.concatenate([pair, moved(pair, other_core)], axis=1)
    peak_all = picked(pair[0], order).reshape(1, shards * rows)
    total_all = picked(pair[1], order).reshape(1, shards * rows)

    def plain(cot, token_ids, args):
        return gradient(jnp.bfloat16, half, *args)

    def crowded_too(cot, token_ids, args):
        my_rows = base + jnp.arange(half, dtype=jnp.int32)

        def step(k, carry):
            total, block = carry
            shard = (z - k) % nz
            for core in range(2):
                if core == 1:
                    block = moved(block, other_core)
                owner = c if core == 0 else 1 - c
                shard_ids = lax.dynamic_slice(
                    token_ids[0].reshape(nz, nc, rows), (shard, owner, 0), (1, 1, rows)
                ).reshape(rows)
                a, b, d = cell_of(shard_ids)
                match = (a == z) & (b == column) & (d == s)
                late = match & (ranks(match[None])[0] >= SLOTS)
                weights = (my_rows[:, None] == jnp.where(late, shard_ids, -1)[None, :]).astype(jnp.bfloat16)
                total = total + dot(weights, block, ((1,), (0,)))
            block = moved(moved(block, other_core), plus_z)
            return total, block

        total, _ = lax.fori_loop(0, nz, step, (gradient(jnp.float32, half, *args), cot))
        return total.astype(jnp.bfloat16)

    args = (base, scores, parts, peak_all, total_all, targets, slots, gots)
    out = lax.cond(crowded, crowded_too, plain, cot, token_ids, args)
    return out.reshape(1, 1, half, width)


def solution(mesh):
    finer = Mesh(mesh.devices.reshape(mesh.shape["section"], 8, 2, 2, 4), AXES)
    in_specs = (P("s", ("z", "c"), None), P(), P(("z", "c", "u", "x"), None))
    out_specs = P(("z", "c", "u", "x"), "s", None, None)
    return jax.shard_map(whole, mesh=finer, in_specs=in_specs, out_specs=out_specs, check_vma=False)
```

```python
import jax
import jax.numpy as jnp
import numpy as np
from jax import lax
from jax.experimental import pallas as pl
from jax.experimental.pallas import tpu as pltpu
from jax.sharding import Mesh
from jax.sharding import PartitionSpec as P


AXES = ("s", "z", "c", "u", "x")
SUBS = 2
SLOTS = 8
CHUNK = 512


def sizes():
    return {a: lax.axis_size(a) for a in AXES}


def moved(block, route):
    n = sizes()
    shape = [n[a] for a in AXES]
    pairs = []
    for at in np.ndindex(*shape):
        to = route(dict(zip(AXES, at)))
        to = tuple(to[a] % n[a] for a in AXES)
        pairs.append((int(np.ravel_multi_index(at, shape)), int(np.ravel_multi_index(to, shape))))
    return lax.ppermute(block, AXES, pairs)


def across(d):
    return {**d, "s": 1 - d["s"], "u": 1 - d["u"]}


def along_z(d):
    return {**d, "z": d["z"] + (1 if (d["x"] + d["c"]) % 2 == 0 else -1)}


def along_x(d):
    return {**d, "x": d["x"] + (-1 if d["c"] == 0 else 1)}


def other_core(d):
    return {**d, "c": 1 - d["c"]}


def plus_z(d):
    return {**d, "z": d["z"] + 1}


def picked(table, index):
    hit = index[:, None] == jnp.arange(table.shape[0], dtype=jnp.int32)[None, :]
    hit = hit.reshape(hit.shape + (1,) * (table.ndim - 1))
    return jnp.sum(jnp.where(hit, table[None], jnp.zeros((), table.dtype)), axis=1)


def shared(value, axes):
    count = lax.axis_size(axes)
    return lax.all_to_all(jnp.broadcast_to(value, (count, *value.shape)), axes, 0, 0, tiled=True)


def joined(pairs):
    peak = jnp.max(pairs[:, 0], axis=0)
    total = jnp.sum(pairs[:, 1] * jnp.exp(pairs[:, 0] - peak[None]), axis=0)
    return jnp.stack([peak, total])


def dot(a, b, dims):
    return lax.dot_general(a, b, (dims, ((), ())), preferred_element_type=jnp.float32)


def anywhere(count):
    return [pl.BlockSpec(memory_space=pl.ANY)] * count


def in_vmem(count):
    return [pl.BlockSpec(memory_space=pltpu.VMEM)] * count


def fetch(sources, targets, sems):
    copies = [pltpu.make_async_copy(a, b, sems.at[k]) for k, (a, b) in enumerate(zip(sources, targets))]
    for copy in copies:
        copy.start()
    return copies


def await_rows(ref, each, count, k, sems, first):
    for j in range(count):
        piece = k * count + j
        view = ref.at[pl.ds(pl.multiple_of(piece * each, each), each), :]
        pltpu.make_async_copy(view, view, sems.at[first + piece]).wait()


def stacked(ref, parts):
    at, views = 0, []
    for part in parts:
        views.append(ref.at[pl.ds(at, part.shape[0]), :])
        at += part.shape[0]
    return views


def score_kernel(count, refs):
    start, table, parts = refs[0], refs[1], refs[2 : 2 + count]
    scores, stats, table_here, rows_here, sems = refs[2 + count :]
    lines = table_here.shape[0]
    mine = table.at[pl.ds(pl.multiple_of(start[0], lines), lines), :]
    copies = fetch([mine, *parts], [table_here, *stacked(rows_here, parts)], sems)
    copies[0].wait()
    each = parts[0].shape[0]

    def step(k, carry):
        await_rows(rows_here, each, CHUNK // each, k, sems, 1)
        at = pl.ds(pl.multiple_of(k * CHUNK, CHUNK), CHUNK)
        value = lax.dot_general(
            table_here[...], rows_here[at, :], (((1,), (1,)), ((), ())), preferred_element_type=jnp.float32
        )
        peak = jnp.max(value, axis=0, keepdims=True)
        value = jnp.exp(value - peak)
        scores[:, at] = value
        stats[0:1, at] = peak
        stats[1:2, at] = jnp.sum(value, axis=0, keepdims=True)
        return carry

    lax.fori_loop(0, rows_here.shape[0] // CHUNK, step, 0)


def scored(start, lines, table, parts):
    count = sum(p.shape[0] for p in parts)
    width = table.shape[1]
    return pl.pallas_call(
        lambda *refs: score_kernel(len(parts), refs),
        out_shape=[
            jax.ShapeDtypeStruct((lines, count), jnp.float32),
            jax.ShapeDtypeStruct((2, count), jnp.float32),
        ],
        in_specs=[pl.BlockSpec(memory_space=pltpu.SMEM)] + anywhere(1 + len(parts)),
        out_specs=in_vmem(2),
        scratch_shapes=[
            pltpu.VMEM((lines, width), table.dtype),
            pltpu.VMEM((count, width), table.dtype),
            pltpu.SemaphoreType.DMA((1 + len(parts),)),
        ],
        cost_estimate=pl.CostEstimate(
            flops=2 * count * lines * width, bytes_accessed=2 * width * (lines + count), transcendentals=0
        ),
        name="score",
    )(start.reshape(1), table, *parts)


def gradient_kernel(count, refs):
    base, factor, targets, slots = refs[:4]
    gots, scores = refs[4:6], refs[6]
    parts = refs[7 : 7 + count]
    out, scores_here, rows_here, got_here, result, outgoing, sems = refs[7 + count :]
    lines, width = out.shape
    tokens, each = rows_here.shape[0], parts[0].shape[0]
    chunks = tokens // CHUNK
    sources, views, order = [*gots], stacked(got_here, gots), stacked(rows_here, parts)
    copies = fetch(sources, views, sems)
    for k in range(chunks):
        at = pl.ds(k * CHUNK, CHUNK)
        pltpu.make_async_copy(scores.at[:, at], scores_here.at[k], sems.at[2 + k]).start()
        for j in range(k * CHUNK // each, (k + 1) * CHUNK // each):
            pltpu.make_async_copy(parts[j], order[j], sems.at[2 + chunks + j]).start()
    for copy in copies:
        copy.wait()
    row = base[0] + lax.broadcasted_iota(jnp.int32, (lines, 1), 0)
    first = jnp.where(row == slots[...], 1.0, 0.0).astype(got_here.dtype)
    span = outgoing.shape[2]
    columns = [slice(k * span, (k + 1) * span) for k in range(width // span)]
    for cols in columns:
        result[:, cols] = jnp.dot(first, got_here[:, cols], preferred_element_type=jnp.float32)

    def step(k, carry):
        pltpu.make_async_copy(scores_here.at[k], scores_here.at[k], sems.at[2 + k]).wait()
        await_rows(rows_here, each, CHUNK // each, k, sems, 2 + chunks)
        at = pl.ds(pl.multiple_of(k * CHUNK, CHUNK), CHUNK)
        hot = jnp.where(row == targets[:, at], 1.0, 0.0)
        weights = (scores_here[k] * factor[:, at] - hot).astype(rows_here.dtype)
        for cols in columns:
            result[:, cols] += jnp.dot(weights, rows_here[at, cols], preferred_element_type=jnp.float32)
        return carry

    lax.fori_loop(0, chunks, step, 0)
    stores = []
    for k, cols in enumerate(columns):
        outgoing[k] = result[:, cols].astype(out.dtype)
        store = pltpu.make_async_copy(
            outgoing.at[k], out.at[:, pl.ds(k * span, span)], sems.at[2 + chunks + count + k]
        )
        store.start()
        stores.append(store)
    for store in stores:
        store.wait()


def gradient(dtype, lines, base, scores, parts, factor, targets, slots, gots):
    tokens, width = factor.shape[1], gots[0].shape[1]
    span, chunks = width // 4, tokens // CHUNK
    return pl.pallas_call(
        lambda *refs: gradient_kernel(len(parts), refs),
        out_shape=jax.ShapeDtypeStruct((lines, width), dtype),
        in_specs=[pl.BlockSpec(memory_space=pltpu.SMEM)] + in_vmem(3) + anywhere(3 + len(parts)),
        out_specs=pl.BlockSpec(memory_space=pl.ANY),
        scratch_shapes=[
            pltpu.VMEM((chunks, lines, CHUNK), jnp.float32),
            pltpu.VMEM((tokens, width), jnp.bfloat16),
            pltpu.VMEM((2 * gots[0].shape[0], width), jnp.bfloat16),
            pltpu.VMEM((lines, width), jnp.float32),
            pltpu.VMEM((width // span, lines, span), dtype),
            pltpu.SemaphoreType.DMA((2 + chunks + len(parts) + width // span,)),
        ],
        cost_estimate=pl.CostEstimate(
            flops=2 * tokens * lines * width, bytes_accessed=2 * width * tokens, transcendentals=0
        ),
        name="gradient",
    )(base.reshape(1), factor, targets, slots, *gots, scores, *parts)


def whole(activations, token_ids, embed_table):
    own_rows = activations[0]
    rows, width = own_rows.shape
    n = sizes()
    nz, nc = n["z"], n["c"]
    s, z, c, u, x = (lax.axis_index(a) for a in AXES)
    column = u * n["x"] + x
    columns = n["u"] * n["x"]
    table_count = embed_table.shape[0]
    half = table_count // n["s"]

    cut = rows // SUBS
    blocks, cots = [], []
    for k in range(SUBS):
        piece = own_rows[k * cut : (k + 1) * cut]
        partner = moved(piece, across)
        if blocks:
            partner, blocks[-1] = lax.optimization_barrier((partner, blocks[-1]))
        blocks.append(jnp.where(s == 0, partner, piece))
        cots.append(jnp.where(s == 0, piece, partner))
    cot = jnp.concatenate(cots, axis=0)

    hops = np.array([0, 1] + [h for step in range(2, nz // 2 + 1) for h in (step, 1 - step)], np.int32)
    way = jnp.where((x + c) % 2 == 0, 1, -1)
    order = []
    for k in range(0, len(hops), 2):
        near = hops[k : k + 2]
        order += [(z - way * near) % nz, (z + way * near) % nz + nz]
    order = jnp.concatenate(order)
    shards = nz * nc

    def both_cores(table):
        table = table.reshape(nz, nc, rows)
        mine = jnp.arange(nc, dtype=jnp.int32)[None, :, None] == c
        return jnp.concatenate(
            [jnp.sum(jnp.where(hit, table, 0), axis=1) for hit in (mine, ~mine)], axis=0
        )

    shard_in, shard_out = both_cores(token_ids[0].reshape(shards, rows)), both_cores(
        token_ids[1].reshape(shards, rows)
    )
    targets = picked(shard_out, order).reshape(1, shards * rows)
    base = ((z * nc + c) * columns + column) * table_count + s * half

    per_z = nc * columns * table_count
    cell_of = lambda v: (v // per_z, (v // table_count) % columns, (v // half) % n["s"])
    before = (
        jnp.arange(rows)[:, None] < jnp.arange(rows)[None, :]
    ).astype(jnp.bfloat16)

    def ranks(match):
        return dot(match.astype(jnp.bfloat16), before, ((1,), (0,))).astype(jnp.int32)

    slot = jnp.arange(SLOTS, dtype=jnp.int32)
    shard_ids = picked(shard_in[:nz], z[None])[0]
    to_z, to_column, to_s = cell_of(shard_ids)
    here = (to_column == column) & (to_s == s)
    out_match = (to_z[None, :] == jnp.arange(nz)[:, None]) & here[None, :]
    out_rank = ranks(out_match)
    every = token_ids[0].reshape(nz * nc, rows)
    cz, cc, cs = cell_of(every)
    cell = (cz * columns + cc) * n["s"] + cs
    cells = nz * columns * n["s"]
    held = jnp.sum(
        (cell[:, :, None] == jnp.arange(cells, dtype=jnp.int32)[None, None, :]).astype(jnp.int32), axis=1
    )
    crowded = jnp.max(held) > SLOTS

    cot, crowded = lax.optimization_barrier((cot, crowded))
    choose = out_match[:, None, :] & (out_rank[:, None, :] == slot[None, :, None])
    sent = dot(choose.reshape(nz * SLOTS, rows).astype(jnp.bfloat16), cot, ((1,), (0,)))
    sent = sent.astype(jnp.bfloat16)
    from_z, from_column, from_s = cell_of(shard_in)
    in_match = (from_z == z) & (from_column == column) & (from_s == s)
    in_rank = ranks(in_match)
    filled = in_match[:, None, :] & (in_rank[:, None, :] == slot[None, :, None])
    slots = jnp.sum(jnp.where(filled, shard_in[:, None, :] + 1, 0), axis=2).reshape(1, shards * SLOTS) - 1

    there, back = [[block] for block in blocks], [[] for _ in blocks]
    for step in range(1, nz // 2 + 1):
        for k in range(SUBS):
            block = there[k][-1]
            if step == 3 and k == 0:
                block, slots, targets, sent = lax.optimization_barrier((block, slots, targets, sent))
            there[k].append(moved(block, along_z))
            if step > 1:
                back[k].append(moved(block, along_x))
    parts = []
    for pair in range(0, len(hops), 2):
        group = []
        for hop in hops[pair : pair + 2]:
            group += [there[k][hop] if hop >= 0 else back[k][-hop - 1] for k in range(SUBS)]
        parts += group + [moved(p, other_core) for p in group]
    got = lax.all_to_all(sent, "z", 0, 0, tiled=True)
    table_scores, stats = scored(s * half, half, embed_table, parts)
    stats, got = lax.optimization_barrier((stats, got))
    scores = table_scores
    gots = (got, moved(got, other_core))

    local = stats.reshape(2, shards, rows)
    place = jnp.arange(shards, dtype=jnp.int32)
    inverse = jnp.sum(jnp.where(order[None, :] == place[:, None], place[None, :], 0), axis=1)
    near = jnp.stack([picked(local[0], inverse[:nz]), picked(local[1], inverse[:nz])])
    far = jnp.stack([picked(local[0], inverse[nz:]), picked(local[1], inverse[nz:])])
    pair = joined(jnp.stack([near, moved(far, other_core)]))
    pair = joined(shared(pair, ("s", "u", "x")))
    pair = joined(shared(pair, "z"))
    pair = jnp.concatenate([pair, moved(pair, other_core)], axis=1)
    factor = jnp.exp(local[0] - picked(pair[0], order)) / picked(pair[1], order)
    factor = factor.reshape(1, shards * rows)

    def plain(cot, token_ids, args):
        return gradient(jnp.bfloat16, half, *args)

    def crowded_too(cot, token_ids, args):
        my_rows = base + jnp.arange(half, dtype=jnp.int32)

        def step(k, carry):
            total, block = carry
            shard = (z - k) % nz
            for core in range(2):
                if core == 1:
                    block = moved(block, other_core)
                owner = c if core == 0 else 1 - c
                shard_ids = lax.dynamic_slice(
                    token_ids[0].reshape(nz, nc, rows), (shard, owner, 0), (1, 1, rows)
                ).reshape(rows)
                a, b, d = cell_of(shard_ids)
                match = (a == z) & (b == column) & (d == s)
                late = match & (ranks(match[None])[0] >= SLOTS)
                weights = (my_rows[:, None] == jnp.where(late, shard_ids, -1)[None, :]).astype(jnp.bfloat16)
                total = total + dot(weights, block, ((1,), (0,)))
            block = moved(moved(block, other_core), plus_z)
            return total, block

        total, _ = lax.fori_loop(0, nz, step, (gradient(jnp.float32, half, *args), cot))
        return total.astype(jnp.bfloat16)

    args = (base, scores, parts, factor, targets, slots, gots)
    out = lax.cond(crowded, crowded_too, plain, cot, token_ids, args)
    return out.reshape(1, 1, half, width)


def solution(mesh):
    finer = Mesh(mesh.devices.reshape(mesh.shape["section"], 8, 2, 2, 4), AXES)
    in_specs = (P("s", ("z", "c"), None), P(), P(("z", "c", "u", "x"), None))
    out_specs = P(("z", "c", "u", "x"), "s", None, None)
    return jax.shard_map(whole, mesh=finer, in_specs=in_specs, out_specs=out_specs, check_vma=False)
```

```python
import jax
import jax.numpy as jnp
import numpy as np
from jax import lax
from jax.experimental import pallas as pl
from jax.experimental.pallas import tpu as pltpu
from jax.sharding import Mesh
from jax.sharding import PartitionSpec as P


AXES = ("s", "z", "c", "u", "x")
SUBS = 2
SLOTS = 8
CHUNK = 512


def sizes():
    return {a: lax.axis_size(a) for a in AXES}


def moved(block, route):
    n = sizes()
    shape = [n[a] for a in AXES]
    pairs = []
    for at in np.ndindex(*shape):
        to = route(dict(zip(AXES, at)))
        to = tuple(to[a] % n[a] for a in AXES)
        pairs.append((int(np.ravel_multi_index(at, shape)), int(np.ravel_multi_index(to, shape))))
    return lax.ppermute(block, AXES, pairs)


def across(d):
    return {**d, "s": 1 - d["s"], "u": 1 - d["u"]}


def along_z(d):
    return {**d, "z": d["z"] + (1 if (d["x"] + d["c"]) % 2 == 0 else -1)}


def along_x(d):
    return {**d, "x": d["x"] + (1 if (d["x"] + d["c"]) % 2 == 0 else -1)}


def other_core(d):
    return {**d, "c": 1 - d["c"]}


def plus_z(d):
    return {**d, "z": d["z"] + 1}


def picked(table, index):
    hit = index[:, None] == jnp.arange(table.shape[0], dtype=jnp.int32)[None, :]
    hit = hit.reshape(hit.shape + (1,) * (table.ndim - 1))
    return jnp.sum(jnp.where(hit, table[None], jnp.zeros((), table.dtype)), axis=1)


def shared(value, axes):
    count = lax.axis_size(axes)
    return lax.all_to_all(jnp.broadcast_to(value, (count, *value.shape)), axes, 0, 0, tiled=True)


def joined(pairs):
    peak = jnp.max(pairs[:, 0], axis=0)
    total = jnp.sum(pairs[:, 1] * jnp.exp(pairs[:, 0] - peak[None]), axis=0)
    return jnp.stack([peak, total])


def dot(a, b, dims):
    return lax.dot_general(a, b, (dims, ((), ())), preferred_element_type=jnp.float32)


def anywhere(count):
    return [pl.BlockSpec(memory_space=pl.ANY)] * count


def in_vmem(count):
    return [pl.BlockSpec(memory_space=pltpu.VMEM)] * count


def fetch(sources, targets, sems):
    copies = [pltpu.make_async_copy(a, b, sems.at[k]) for k, (a, b) in enumerate(zip(sources, targets))]
    for copy in copies:
        copy.start()
    return copies


def await_rows(ref, each, count, k, sems, first):
    for j in range(count):
        piece = k * count + j
        view = ref.at[pl.ds(pl.multiple_of(piece * each, each), each), :]
        pltpu.make_async_copy(view, view, sems.at[first + piece]).wait()


def stacked(ref, parts):
    at, views = 0, []
    for part in parts:
        views.append(ref.at[pl.ds(at, part.shape[0]), :])
        at += part.shape[0]
    return views


def score_kernel(count, refs):
    start, table, parts = refs[0], refs[1], refs[2 : 2 + count]
    scores, stats, table_here, rows_here, sems = refs[2 + count :]
    lines = table_here.shape[0]
    mine = table.at[pl.ds(pl.multiple_of(start[0], lines), lines), :]
    copies = fetch([mine, *parts], [table_here, *stacked(rows_here, parts)], sems)
    copies[0].wait()
    each = parts[0].shape[0]

    def step(k, carry):
        await_rows(rows_here, each, CHUNK // each, k, sems, 1)
        at = pl.ds(pl.multiple_of(k * CHUNK, CHUNK), CHUNK)
        value = lax.dot_general(
            table_here[...], rows_here[at, :], (((1,), (1,)), ((), ())), preferred_element_type=jnp.float32
        )
        peak = jnp.max(value, axis=0, keepdims=True)
        value = jnp.exp(value - peak)
        scores[:, at] = value
        stats[0:1, at] = peak
        stats[1:2, at] = jnp.sum(value, axis=0, keepdims=True)
        return carry

    lax.fori_loop(0, rows_here.shape[0] // CHUNK, step, 0)


def scored(start, lines, table, parts):
    count = sum(p.shape[0] for p in parts)
    width = table.shape[1]
    return pl.pallas_call(
        lambda *refs: score_kernel(len(parts), refs),
        out_shape=[
            jax.ShapeDtypeStruct((lines, count), jnp.float32),
            jax.ShapeDtypeStruct((2, count), jnp.float32),
        ],
        in_specs=[pl.BlockSpec(memory_space=pltpu.SMEM)] + anywhere(1 + len(parts)),
        out_specs=in_vmem(2),
        scratch_shapes=[
            pltpu.VMEM((lines, width), table.dtype),
            pltpu.VMEM((count, width), table.dtype),
            pltpu.SemaphoreType.DMA((1 + len(parts),)),
        ],
        cost_estimate=pl.CostEstimate(
            flops=2 * count * lines * width, bytes_accessed=2 * width * (lines + count), transcendentals=0
        ),
        name="score",
    )(start.reshape(1), table, *parts)


def gradient_kernel(count, refs):
    base, factor, targets, slots = refs[:4]
    gots, scores = refs[4:6], refs[6]
    parts = refs[7 : 7 + count]
    out, scores_here, rows_here, got_here, result, outgoing, sems = refs[7 + count :]
    lines, width = out.shape
    tokens, each = rows_here.shape[0], parts[0].shape[0]
    chunks = tokens // CHUNK
    sources, views, order = [*gots], stacked(got_here, gots), stacked(rows_here, parts)
    copies = fetch(sources, views, sems)
    for k in range(chunks):
        at = pl.ds(k * CHUNK, CHUNK)
        pltpu.make_async_copy(scores.at[:, at], scores_here.at[k], sems.at[2 + k]).start()
        for j in range(k * CHUNK // each, (k + 1) * CHUNK // each):
            pltpu.make_async_copy(parts[j], order[j], sems.at[2 + chunks + j]).start()
    for copy in copies:
        copy.wait()
    row = base[0] + lax.broadcasted_iota(jnp.int32, (lines, 1), 0)
    first = jnp.where(row == slots[...], 1.0, 0.0).astype(got_here.dtype)
    span = outgoing.shape[2]
    columns = [slice(k * span, (k + 1) * span) for k in range(width // span)]
    for cols in columns:
        result[:, cols] = jnp.dot(first, got_here[:, cols], preferred_element_type=jnp.float32)

    def step(k, carry):
        pltpu.make_async_copy(scores_here.at[k], scores_here.at[k], sems.at[2 + k]).wait()
        await_rows(rows_here, each, CHUNK // each, k, sems, 2 + chunks)
        at = pl.ds(pl.multiple_of(k * CHUNK, CHUNK), CHUNK)
        hot = jnp.where(row == targets[:, at], 1.0, 0.0)
        weights = (scores_here[k] * factor[:, at] - hot).astype(rows_here.dtype)
        for cols in columns:
            result[:, cols] += jnp.dot(weights, rows_here[at, cols], preferred_element_type=jnp.float32)
        return carry

    lax.fori_loop(0, chunks, step, 0)
    stores = []
    for k, cols in enumerate(columns):
        outgoing[k] = result[:, cols].astype(out.dtype)
        store = pltpu.make_async_copy(
            outgoing.at[k], out.at[:, pl.ds(k * span, span)], sems.at[2 + chunks + count + k]
        )
        store.start()
        stores.append(store)
    for store in stores:
        store.wait()


def gradient(dtype, lines, base, scores, parts, factor, targets, slots, gots):
    tokens, width = factor.shape[1], gots[0].shape[1]
    span, chunks = width // 4, tokens // CHUNK
    return pl.pallas_call(
        lambda *refs: gradient_kernel(len(parts), refs),
        out_shape=jax.ShapeDtypeStruct((lines, width), dtype),
        in_specs=[pl.BlockSpec(memory_space=pltpu.SMEM)] + in_vmem(3) + anywhere(3 + len(parts)),
        out_specs=pl.BlockSpec(memory_space=pl.ANY),
        scratch_shapes=[
            pltpu.VMEM((chunks, lines, CHUNK), jnp.float32),
            pltpu.VMEM((tokens, width), jnp.bfloat16),
            pltpu.VMEM((2 * gots[0].shape[0], width), jnp.bfloat16),
            pltpu.VMEM((lines, width), jnp.float32),
            pltpu.VMEM((width // span, lines, span), dtype),
            pltpu.SemaphoreType.DMA((2 + chunks + len(parts) + width // span,)),
        ],
        cost_estimate=pl.CostEstimate(
            flops=2 * tokens * lines * width, bytes_accessed=2 * width * tokens, transcendentals=0
        ),
        name="gradient",
    )(base.reshape(1), factor, targets, slots, *gots, scores, *parts)


def whole(activations, token_ids, embed_table):
    own_rows = activations[0]
    rows, width = own_rows.shape
    n = sizes()
    nz, nc = n["z"], n["c"]
    s, z, c, u, x = (lax.axis_index(a) for a in AXES)
    column = u * n["x"] + x
    columns = n["u"] * n["x"]
    table_count = embed_table.shape[0]
    half = table_count // n["s"]

    cut = rows // SUBS
    blocks, cots = [], []
    for k in range(SUBS):
        piece = own_rows[k * cut : (k + 1) * cut]
        partner = moved(piece, across)
        if blocks:
            partner, blocks[-1] = lax.optimization_barrier((partner, blocks[-1]))
        blocks.append(jnp.where(s == 0, partner, piece))
        cots.append(jnp.where(s == 0, piece, partner))
    cot = jnp.concatenate(cots, axis=0)

    hops = np.array([0, 1] + [h for step in range(2, nz // 2 + 1) for h in (step, 1 - step)], np.int32)
    way = jnp.where((x + c) % 2 == 0, 1, -1)
    order = []
    for k in range(0, len(hops), 2):
        near = hops[k : k + 2]
        order += [(z - way * near) % nz, (z + way * near) % nz + nz]
    order = jnp.concatenate(order)
    shards = nz * nc

    def both_cores(table):
        table = table.reshape(nz, nc, rows)
        mine = jnp.arange(nc, dtype=jnp.int32)[None, :, None] == c
        return jnp.concatenate(
            [jnp.sum(jnp.where(hit, table, 0), axis=1) for hit in (mine, ~mine)], axis=0
        )

    shard_in, shard_out = both_cores(token_ids[0].reshape(shards, rows)), both_cores(
        token_ids[1].reshape(shards, rows)
    )
    targets = picked(shard_out, order).reshape(1, shards * rows)
    base = ((z * nc + c) * columns + column) * table_count + s * half

    per_z = nc * columns * table_count
    cell_of = lambda v: (v // per_z, (v // table_count) % columns, (v // half) % n["s"])
    before = (
        jnp.arange(rows)[:, None] < jnp.arange(rows)[None, :]
    ).astype(jnp.bfloat16)

    def ranks(match):
        return dot(match.astype(jnp.bfloat16), before, ((1,), (0,))).astype(jnp.int32)

    slot = jnp.arange(SLOTS, dtype=jnp.int32)
    shard_ids = picked(shard_in[:nz], z[None])[0]
    to_z, to_column, to_s = cell_of(shard_ids)
    here = (to_column == column) & (to_s == s)
    out_match = (to_z[None, :] == jnp.arange(nz)[:, None]) & here[None, :]
    out_rank = ranks(out_match)
    every = token_ids[0].reshape(nz * nc, rows)
    cz, cc, cs = cell_of(every)
    cell = (cz * columns + cc) * n["s"] + cs
    cells = nz * columns * n["s"]
    held = jnp.sum(
        (cell[:, :, None] == jnp.arange(cells, dtype=jnp.int32)[None, None, :]).astype(jnp.int32), axis=1
    )
    crowded = jnp.max(held) > SLOTS

    cot, crowded = lax.optimization_barrier((cot, crowded))
    choose = out_match[:, None, :] & (out_rank[:, None, :] == slot[None, :, None])
    sent = dot(choose.reshape(nz * SLOTS, rows).astype(jnp.bfloat16), cot, ((1,), (0,)))
    sent = sent.astype(jnp.bfloat16)
    from_z, from_column, from_s = cell_of(shard_in)
    in_match = (from_z == z) & (from_column == column) & (from_s == s)
    in_rank = ranks(in_match)
    filled = in_match[:, None, :] & (in_rank[:, None, :] == slot[None, :, None])
    slots = jnp.sum(jnp.where(filled, shard_in[:, None, :] + 1, 0), axis=2).reshape(1, shards * SLOTS) - 1

    there, back = [[block] for block in blocks], [[] for _ in blocks]
    for step in range(1, nz // 2 + 1):
        for k in range(SUBS):
            block = there[k][-1]
            if step == 3 and k == 0:
                block, slots, targets, sent = lax.optimization_barrier((block, slots, targets, sent))
            there[k].append(moved(block, along_z))
            if step > 1:
                back[k].append(moved(block, along_x))
    early = []
    for k in range(SUBS):
        early.append(moved(blocks[k], other_core))
    parts = []
    for pair in range(0, len(hops), 2):
        group = []
        for hop in hops[pair : pair + 2]:
            group += [there[k][hop] if hop >= 0 else back[k][-hop - 1] for k in range(SUBS)]
        if pair == 0:
            parts += group + early + [moved(p, other_core) for p in group[SUBS:]]
        else:
            parts += group + [moved(p, other_core) for p in group]
    got = lax.all_to_all(sent, "z", 0, 0, tiled=True)
    table_scores, stats = scored(s * half, half, embed_table, parts)
    stats, got = lax.optimization_barrier((stats, got))
    scores = table_scores
    gots = (got, moved(got, other_core))

    local = stats.reshape(2, shards, rows)
    place = jnp.arange(shards, dtype=jnp.int32)
    inverse = jnp.sum(jnp.where(order[None, :] == place[:, None], place[None, :], 0), axis=1)
    near = jnp.stack([picked(local[0], inverse[:nz]), picked(local[1], inverse[:nz])])
    far = jnp.stack([picked(local[0], inverse[nz:]), picked(local[1], inverse[nz:])])
    pair = joined(jnp.stack([near, moved(far, other_core)]))
    pair = joined(shared(pair, ("s", "u", "x")))
    pair = joined(shared(pair, "z"))
    pair = jnp.concatenate([pair, moved(pair, other_core)], axis=1)
    factor = jnp.exp(local[0] - picked(pair[0], order)) / picked(pair[1], order)
    factor = factor.reshape(1, shards * rows)

    def plain(cot, token_ids, args):
        return gradient(jnp.bfloat16, half, *args)

    def crowded_too(cot, token_ids, args):
        my_rows = base + jnp.arange(half, dtype=jnp.int32)

        def step(k, carry):
            total, block = carry
            shard = (z - k) % nz
            for core in range(2):
                if core == 1:
                    block = moved(block, other_core)
                owner = c if core == 0 else 1 - c
                shard_ids = lax.dynamic_slice(
                    token_ids[0].reshape(nz, nc, rows), (shard, owner, 0), (1, 1, rows)
                ).reshape(rows)
                a, b, d = cell_of(shard_ids)
                match = (a == z) & (b == column) & (d == s)
                late = match & (ranks(match[None])[0] >= SLOTS)
                weights = (my_rows[:, None] == jnp.where(late, shard_ids, -1)[None, :]).astype(jnp.bfloat16)
                total = total + dot(weights, block, ((1,), (0,)))
            block = moved(moved(block, other_core), plus_z)
            return total, block

        total, _ = lax.fori_loop(0, nz, step, (gradient(jnp.float32, half, *args), cot))
        return total.astype(jnp.bfloat16)

    args = (base, scores, parts, factor, targets, slots, gots)
    out = lax.cond(crowded, crowded_too, plain, cot, token_ids, args)
    return out.reshape(1, 1, half, width)


def solution(mesh):
    finer = Mesh(mesh.devices.reshape(mesh.shape["section"], 8, 2, 2, 4), AXES)
    in_specs = (P("s", ("z", "c"), None), P(), P(("z", "c", "u", "x"), None))
    out_specs = P(("z", "c", "u", "x"), "s", None, None)
    return jax.shard_map(whole, mesh=finer, in_specs=in_specs, out_specs=out_specs, check_vma=False)
```

```python
import jax
import jax.numpy as jnp
import numpy as np
from jax import lax
from jax.experimental import pallas as pl
from jax.experimental.pallas import tpu as pltpu
from jax.sharding import Mesh
from jax.sharding import PartitionSpec as P


AXES = ("s", "z", "c", "u", "x")
SUBS = 2
SLOTS = 8
CHUNK = 512


def sizes():
    return {a: lax.axis_size(a) for a in AXES}


def moved(block, route):
    n = sizes()
    shape = [n[a] for a in AXES]
    pairs = []
    for at in np.ndindex(*shape):
        to = route(dict(zip(AXES, at)))
        to = tuple(to[a] % n[a] for a in AXES)
        pairs.append((int(np.ravel_multi_index(at, shape)), int(np.ravel_multi_index(to, shape))))
    return lax.ppermute(block, AXES, pairs)


def across(d):
    return {**d, "s": 1 - d["s"], "u": 1 - d["u"]}


def along_z(d):
    return {**d, "z": d["z"] + (1 if (d["x"] + d["c"]) % 2 == 0 else -1)}


def along_x(d):
    return {**d, "x": d["x"] + (1 if (d["x"] + d["c"]) % 2 == 0 else -1)}


def other_core(d):
    return {**d, "c": 1 - d["c"]}


def plus_z(d):
    return {**d, "z": d["z"] + 1}


def picked(table, index):
    hit = index[:, None] == jnp.arange(table.shape[0], dtype=jnp.int32)[None, :]
    hit = hit.reshape(hit.shape + (1,) * (table.ndim - 1))
    return jnp.sum(jnp.where(hit, table[None], jnp.zeros((), table.dtype)), axis=1)


def shared(value, axes):
    count = lax.axis_size(axes)
    return lax.all_to_all(jnp.broadcast_to(value, (count, *value.shape)), axes, 0, 0, tiled=True)


def joined(pairs):
    peak = jnp.max(pairs[:, 0], axis=0)
    total = jnp.sum(pairs[:, 1] * jnp.exp(pairs[:, 0] - peak[None]), axis=0)
    return jnp.stack([peak, total])


def dot(a, b, dims):
    return lax.dot_general(a, b, (dims, ((), ())), preferred_element_type=jnp.float32)


def anywhere(count):
    return [pl.BlockSpec(memory_space=pl.ANY)] * count


def in_vmem(count):
    return [pl.BlockSpec(memory_space=pltpu.VMEM)] * count


def fetch(sources, targets, sems):
    copies = [pltpu.make_async_copy(a, b, sems.at[k]) for k, (a, b) in enumerate(zip(sources, targets))]
    for copy in copies:
        copy.start()
    return copies


def await_rows(ref, each, count, k, sems, first):
    for j in range(count):
        piece = k * count + j
        view = ref.at[pl.ds(pl.multiple_of(piece * each, each), each), :]
        pltpu.make_async_copy(view, view, sems.at[first + piece]).wait()


def stacked(ref, parts):
    at, views = 0, []
    for part in parts:
        views.append(ref.at[pl.ds(at, part.shape[0]), :])
        at += part.shape[0]
    return views


def score_kernel(count, refs):
    start, table, parts = refs[0], refs[1], refs[2 : 2 + count]
    scores, stats, table_here, rows_here, sems = refs[2 + count :]
    lines = table_here.shape[0]
    mine = table.at[pl.ds(pl.multiple_of(start[0], lines), lines), :]
    copies = fetch([mine, *parts], [table_here, *stacked(rows_here, parts)], sems)
    copies[0].wait()
    each = parts[0].shape[0]

    def step(k, carry):
        await_rows(rows_here, each, CHUNK // each, k, sems, 1)
        at = pl.ds(pl.multiple_of(k * CHUNK, CHUNK), CHUNK)
        value = lax.dot_general(
            table_here[...], rows_here[at, :], (((1,), (1,)), ((), ())), preferred_element_type=jnp.float32
        )
        peak = jnp.max(value, axis=0, keepdims=True)
        value = jnp.exp(value - peak)
        scores[:, at] = value
        stats[0:1, at] = peak
        stats[1:2, at] = jnp.sum(value, axis=0, keepdims=True)
        return carry

    lax.fori_loop(0, rows_here.shape[0] // CHUNK, step, 0)


def scored(start, lines, table, parts):
    count = sum(p.shape[0] for p in parts)
    width = table.shape[1]
    return pl.pallas_call(
        lambda *refs: score_kernel(len(parts), refs),
        out_shape=[
            jax.ShapeDtypeStruct((lines, count), jnp.float32),
            jax.ShapeDtypeStruct((2, count), jnp.float32),
        ],
        in_specs=[pl.BlockSpec(memory_space=pltpu.SMEM)] + anywhere(1 + len(parts)),
        out_specs=in_vmem(2),
        scratch_shapes=[
            pltpu.VMEM((lines, width), table.dtype),
            pltpu.VMEM((count, width), table.dtype),
            pltpu.SemaphoreType.DMA((1 + len(parts),)),
        ],
        cost_estimate=pl.CostEstimate(
            flops=2 * count * lines * width, bytes_accessed=2 * width * (lines + count), transcendentals=0
        ),
        name="score",
    )(start.reshape(1), table, *parts)


def gradient_kernel(count, refs):
    base, factor, targets, slots = refs[:4]
    gots, scores = refs[4:6], refs[6]
    parts = refs[7 : 7 + count]
    out, scores_here, rows_here, got_here, result, outgoing, sems = refs[7 + count :]
    lines, width = out.shape
    tokens, each = rows_here.shape[0], parts[0].shape[0]
    chunks = tokens // CHUNK
    sources, views, order = [*gots], stacked(got_here, gots), stacked(rows_here, parts)
    copies = fetch(sources, views, sems)
    for k in range(chunks):
        at = pl.ds(k * CHUNK, CHUNK)
        pltpu.make_async_copy(scores.at[:, at], scores_here.at[k], sems.at[2 + k]).start()
        for j in range(k * CHUNK // each, (k + 1) * CHUNK // each):
            pltpu.make_async_copy(parts[j], order[j], sems.at[2 + chunks + j]).start()
    for copy in copies:
        copy.wait()
    row = base[0] + lax.broadcasted_iota(jnp.int32, (lines, 1), 0)
    first = jnp.where(row == slots[...], 1.0, 0.0).astype(got_here.dtype)
    span = outgoing.shape[2]
    columns = [slice(k * span, (k + 1) * span) for k in range(width // span)]
    for cols in columns:
        result[:, cols] = jnp.dot(first, got_here[:, cols], preferred_element_type=jnp.float32)

    def step(k, carry):
        pltpu.make_async_copy(scores_here.at[k], scores_here.at[k], sems.at[2 + k]).wait()
        await_rows(rows_here, each, CHUNK // each, k, sems, 2 + chunks)
        at = pl.ds(pl.multiple_of(k * CHUNK, CHUNK), CHUNK)
        hot = jnp.where(row == targets[:, at], 1.0, 0.0)
        weights = (scores_here[k] * factor[:, at] - hot).astype(rows_here.dtype)
        for cols in columns:
            result[:, cols] += jnp.dot(weights, rows_here[at, cols], preferred_element_type=jnp.float32)
        return carry

    lax.fori_loop(0, chunks, step, 0)
    stores = []
    for k, cols in enumerate(columns):
        outgoing[k] = result[:, cols].astype(out.dtype)
        store = pltpu.make_async_copy(
            outgoing.at[k], out.at[:, pl.ds(k * span, span)], sems.at[2 + chunks + count + k]
        )
        store.start()
        stores.append(store)
    for store in stores:
        store.wait()


def gradient(dtype, lines, base, scores, parts, factor, targets, slots, gots):
    tokens, width = factor.shape[1], gots[0].shape[1]
    span, chunks = width // 4, tokens // CHUNK
    return pl.pallas_call(
        lambda *refs: gradient_kernel(len(parts), refs),
        out_shape=jax.ShapeDtypeStruct((lines, width), dtype),
        in_specs=[pl.BlockSpec(memory_space=pltpu.SMEM)] + in_vmem(3) + anywhere(3 + len(parts)),
        out_specs=pl.BlockSpec(memory_space=pl.ANY),
        scratch_shapes=[
            pltpu.VMEM((chunks, lines, CHUNK), jnp.float32),
            pltpu.VMEM((tokens, width), jnp.bfloat16),
            pltpu.VMEM((2 * gots[0].shape[0], width), jnp.bfloat16),
            pltpu.VMEM((lines, width), jnp.float32),
            pltpu.VMEM((width // span, lines, span), dtype),
            pltpu.SemaphoreType.DMA((2 + chunks + len(parts) + width // span,)),
        ],
        cost_estimate=pl.CostEstimate(
            flops=2 * tokens * lines * width, bytes_accessed=2 * width * tokens, transcendentals=0
        ),
        name="gradient",
    )(base.reshape(1), factor, targets, slots, *gots, scores, *parts)


def whole(activations, token_ids, embed_table):
    own_rows = activations[0]
    rows, width = own_rows.shape
    n = sizes()
    nz, nc = n["z"], n["c"]
    s, z, c, u, x = (lax.axis_index(a) for a in AXES)
    column = u * n["x"] + x
    columns = n["u"] * n["x"]
    table_count = embed_table.shape[0]
    half = table_count // n["s"]

    cut = rows // SUBS
    blocks, cots = [], []
    for k in range(SUBS):
        piece = own_rows[k * cut : (k + 1) * cut]
        partner = moved(piece, across)
        if blocks:
            partner, blocks[-1] = lax.optimization_barrier((partner, blocks[-1]))
        blocks.append(jnp.where(s == 0, partner, piece))
        cots.append(jnp.where(s == 0, piece, partner))
    cot = jnp.concatenate(cots, axis=0)

    hops = np.array([0, 1] + [h for step in range(2, nz // 2 + 1) for h in (step, 1 - step)], np.int32)
    way = jnp.where((x + c) % 2 == 0, 1, -1)
    order = []
    for k in range(0, len(hops), 2):
        near = hops[k : k + 2]
        order += [(z - way * near) % nz, (z + way * near) % nz + nz]
    order = jnp.concatenate(order)
    shards = nz * nc

    def both_cores(table):
        table = table.reshape(nz, nc, rows)
        mine = jnp.arange(nc, dtype=jnp.int32)[None, :, None] == c
        return jnp.concatenate(
            [jnp.sum(jnp.where(hit, table, 0), axis=1) for hit in (mine, ~mine)], axis=0
        )

    shard_in, shard_out = both_cores(token_ids[0].reshape(shards, rows)), both_cores(
        token_ids[1].reshape(shards, rows)
    )
    targets = picked(shard_out, order).reshape(1, shards * rows)
    base = ((z * nc + c) * columns + column) * table_count + s * half

    per_z = nc * columns * table_count
    cell_of = lambda v: (v // per_z, (v // table_count) % columns, (v // half) % n["s"])
    before = (
        jnp.arange(rows)[:, None] < jnp.arange(rows)[None, :]
    ).astype(jnp.bfloat16)

    def ranks(match):
        return dot(match.astype(jnp.bfloat16), before, ((1,), (0,))).astype(jnp.int32)

    slot = jnp.arange(SLOTS, dtype=jnp.int32)
    shard_ids = picked(shard_in[:nz], z[None])[0]
    to_z, to_column, to_s = cell_of(shard_ids)
    here = (to_column == column) & (to_s == s)
    out_match = (to_z[None, :] == jnp.arange(nz)[:, None]) & here[None, :]
    out_rank = ranks(out_match)
    every = token_ids[0].reshape(nz * nc, rows)
    cz, cc, cs = cell_of(every)
    cell = (cz * columns + cc) * n["s"] + cs
    cells = nz * columns * n["s"]
    held = jnp.sum(
        (cell[:, :, None] == jnp.arange(cells, dtype=jnp.int32)[None, None, :]).astype(jnp.int32), axis=1
    )
    crowded = jnp.max(held) > SLOTS

    cot, crowded = lax.optimization_barrier((cot, crowded))
    choose = out_match[:, None, :] & (out_rank[:, None, :] == slot[None, :, None])
    sent = dot(choose.reshape(nz * SLOTS, rows).astype(jnp.bfloat16), cot, ((1,), (0,)))
    sent = sent.astype(jnp.bfloat16)
    from_z, from_column, from_s = cell_of(shard_in)
    in_match = (from_z == z) & (from_column == column) & (from_s == s)
    in_rank = ranks(in_match)
    filled = in_match[:, None, :] & (in_rank[:, None, :] == slot[None, :, None])
    slots = jnp.sum(jnp.where(filled, shard_in[:, None, :] + 1, 0), axis=2).reshape(1, shards * SLOTS) - 1

    there, back = [[block] for block in blocks], [[] for _ in blocks]
    for step in range(1, nz // 2 + 1):
        for k in range(SUBS):
            block = there[k][-1]
            if step == 3 and k == 0:
                block, slots, targets, sent = lax.optimization_barrier((block, slots, targets, sent))
            there[k].append(moved(block, along_z))
            if step > 1:
                back[k].append(moved(block, along_x))
    early = []
    for k in range(SUBS):
        early.append(moved(blocks[k], other_core))
    parts = []
    for pair in range(0, len(hops), 2):
        group = []
        for hop in hops[pair : pair + 2]:
            group += [there[k][hop] if hop >= 0 else back[k][-hop - 1] for k in range(SUBS)]
        if pair == 0:
            parts += group + early + [moved(p, other_core) for p in group[SUBS:]]
        else:
            parts += group + [moved(p, other_core) for p in group]
    got = lax.all_to_all(sent, "z", 0, 0, tiled=True)
    table_scores, stats = scored(s * half, half, embed_table, parts)
    stats, got = lax.optimization_barrier((stats, got))
    scores = table_scores
    gots = (got, moved(got, other_core))

    local = stats.reshape(2, shards, rows)
    place = jnp.arange(shards, dtype=jnp.int32)
    inverse = jnp.sum(jnp.where(order[None, :] == place[:, None], place[None, :], 0), axis=1)
    near = jnp.stack([picked(local[0], inverse[:nz]), picked(local[1], inverse[:nz])])
    far = jnp.stack([picked(local[0], inverse[nz:]), picked(local[1], inverse[nz:])])
    each = jnp.stack([jnp.where(c == core, near, far) for core in range(2)])
    fan = (n["s"], nc, n["u"] * n["x"], *near.shape)
    each = jnp.broadcast_to(each[None, :, None], fan).reshape(-1, *near.shape)
    pair = joined(lax.all_to_all(each, ("s", "c", "u", "x"), 0, 0, tiled=True))
    both = shared(pair, ("z", "c")).reshape(nz, nc, *pair.shape)
    both = jnp.where(c == 0, both, both[:, ::-1])
    pair = jnp.concatenate([joined(both[:, core]) for core in range(2)], axis=1)
    factor = jnp.exp(local[0] - picked(pair[0], order)) / picked(pair[1], order)
    factor = factor.reshape(1, shards * rows)

    def plain(cot, token_ids, args):
        return gradient(jnp.bfloat16, half, *args)

    def crowded_too(cot, token_ids, args):
        my_rows = base + jnp.arange(half, dtype=jnp.int32)

        def step(k, carry):
            total, block = carry
            shard = (z - k) % nz
            for core in range(2):
                if core == 1:
                    block = moved(block, other_core)
                owner = c if core == 0 else 1 - c
                shard_ids = lax.dynamic_slice(
                    token_ids[0].reshape(nz, nc, rows), (shard, owner, 0), (1, 1, rows)
                ).reshape(rows)
                a, b, d = cell_of(shard_ids)
                match = (a == z) & (b == column) & (d == s)
                late = match & (ranks(match[None])[0] >= SLOTS)
                weights = (my_rows[:, None] == jnp.where(late, shard_ids, -1)[None, :]).astype(jnp.bfloat16)
                total = total + dot(weights, block, ((1,), (0,)))
            block = moved(moved(block, other_core), plus_z)
            return total, block

        total, _ = lax.fori_loop(0, nz, step, (gradient(jnp.float32, half, *args), cot))
        return total.astype(jnp.bfloat16)

    args = (base, scores, parts, factor, targets, slots, gots)
    out = lax.cond(crowded, crowded_too, plain, cot, token_ids, args)
    return out.reshape(1, 1, half, width)


def solution(mesh):
    finer = Mesh(mesh.devices.reshape(mesh.shape["section"], 8, 2, 2, 4), AXES)
    in_specs = (P("s", ("z", "c"), None), P(), P(("z", "c", "u", "x"), None))
    out_specs = P(("z", "c", "u", "x"), "s", None, None)
    return jax.shard_map(whole, mesh=finer, in_specs=in_specs, out_specs=out_specs, check_vma=False)
```
